16 devices in a mesh: dp: 2 (over y, z), tp: 8 (over x, core).
Axes of the slice: x: 4, y: 2, z: 1, core: 2. Of those that a mesh axis runs over, the one named last changes fastest.
The devices are a block of a 4x4x8 slice.
Arguments:
- x_resid: bfloat16 [64, 512, 2560], P('dp', 'tp'), parts along dimension 0
- positions: int32 [64, 512], P('dp', 'tp'), parts along dimension 0
- norm_gain: bfloat16 [2560], replicated
- w_q: bfloat16 [2560, 4096], P(None, 'tp')
- w_k: bfloat16 [2560, 1024], P(None, 'tp')
- w_v: bfloat16 [2560, 1024], P(None, 'tp')
- q_gain: bfloat16 [128], replicated
- k_gain: bfloat16 [128], replicated
- w_o: bfloat16 [4096, 2560], P('tp')
Outputs:
- output: bfloat16 [64, 512, 2560], P('dp', 'tp'), parts along dimension 0
There are 2 independent parts. The reference program is written for one: setup_inputs(seed, part) draws one part's arguments, and reference() takes and returns one part's arrays. A program takes and returns all parts, laid end to end along the dimension named above; an argument that names none is the same for every part.
All inputs are finite; a program needn't handle non-finite values.
Results may differ from the reference program's by a relative error of at most 0.012307.
Values are sent between devices in bfloat16 or wider.
A program may use at most 768 MiB of HBM per device.

```python
import jax
import jax.numpy as jnp
from jax import lax

BATCH = 32
SEQ_LEN = 512
D_MODEL = 2560
HEADS = 32
KV_HEADS = 8
HEAD_DIM = 128
Q_BLOCK = 64

GROUP_SIZE = HEADS // KV_HEADS
EPS = 1e-6
THETA = 1000000.0


def setup_inputs(seed: int = 0, part: int = 0) -> dict:
    base_key = jax.random.key(seed)
    shared_keys = jax.random.split(base_key, 8)
    part_keys = jax.random.split(jax.random.fold_in(base_key, part), 3)
    x_in = jax.random.normal(part_keys[0], (BATCH, SEQ_LEN, D_MODEL), jnp.float32)
    start_pos = jax.random.randint(part_keys[1], (BATCH, 1), 0, 1024)
    pos_steps = jax.random.randint(part_keys[2], (BATCH, SEQ_LEN), 1, 4)
    pos_vals = (start_pos + jnp.cumsum(pos_steps, axis=1)).astype(jnp.int32)
    proj_scale = D_MODEL ** -0.5
    out_scale = (HEADS * HEAD_DIM) ** -0.5
    return {
        'x_resid': x_in.astype(jnp.bfloat16),
        'positions': pos_vals,
        'norm_gain': jax.random.uniform(shared_keys[0], (D_MODEL,), jnp.float32, 0.5, 1.5).astype(jnp.bfloat16),
        'w_q': (jax.random.normal(shared_keys[1], (D_MODEL, HEADS * HEAD_DIM), jnp.float32) * proj_scale).astype(jnp.bfloat16),
        'w_k': (jax.random.normal(shared_keys[2], (D_MODEL, KV_HEADS * HEAD_DIM), jnp.float32) * proj_scale).astype(jnp.bfloat16),
        'w_v': (jax.random.normal(shared_keys[3], (D_MODEL, KV_HEADS * HEAD_DIM), jnp.float32) * proj_scale).astype(jnp.bfloat16),
        'q_gain': jax.random.uniform(shared_keys[4], (HEAD_DIM,), jnp.float32, 1.2, 2.0).astype(jnp.bfloat16),
        'k_gain': jax.random.uniform(shared_keys[5], (HEAD_DIM,), jnp.float32, 1.2, 2.0).astype(jnp.bfloat16),
        'w_o': (jax.random.normal(shared_keys[6], (HEADS * HEAD_DIM, D_MODEL), jnp.float32) * out_scale).astype(jnp.bfloat16),
    }


def rms_scale(vals, gain):
    mean_sq = jnp.mean(vals * vals, axis=-1, keepdims=True)
    return vals * lax.rsqrt(mean_sq + EPS) * gain.astype(jnp.float32)


def rotate_half(vals, cos_t, sin_t):
    half_dim = HEAD_DIM // 2
    lower_half = vals[..., :half_dim]
    upper_half = vals[..., half_dim:]
    return jnp.concatenate([lower_half * cos_t - upper_half * sin_t, upper_half * cos_t + lower_half * sin_t], axis=-1)


def reference(x_resid, positions, norm_gain, w_q, w_k, w_v, q_gain, k_gain, w_o):
    inv_freq = THETA ** (-(jnp.arange(HEAD_DIM // 2, dtype=jnp.float32) * (2.0 / HEAD_DIM)))
    key_index = jnp.arange(SEQ_LEN)
    block_starts = jnp.arange(SEQ_LEN // Q_BLOCK) * Q_BLOCK

    def one_sequence(seq_args):
        x_seq, pos_seq = seq_args
        x_f32 = x_seq.astype(jnp.float32)
        normed = rms_scale(x_f32, norm_gain).astype(jnp.bfloat16)
        q_proj = jnp.dot(normed, w_q, preferred_element_type=jnp.float32).astype(jnp.bfloat16)
        k_proj = jnp.dot(normed, w_k, preferred_element_type=jnp.float32).astype(jnp.bfloat16)
        v_proj = jnp.dot(normed, w_v, preferred_element_type=jnp.float32).astype(jnp.bfloat16)
        angles = pos_seq.astype(jnp.float32)[:, None] * inv_freq
        cos_t = jnp.cos(angles)
        sin_t = jnp.sin(angles)
        q_heads = q_proj.reshape(SEQ_LEN, KV_HEADS, GROUP_SIZE, HEAD_DIM).astype(jnp.float32)
        k_heads = k_proj.reshape(SEQ_LEN, KV_HEADS, HEAD_DIM).astype(jnp.float32)
        q_rot = rotate_half(rms_scale(q_heads, q_gain), cos_t[:, None, None, :], sin_t[:, None, None, :]).astype(jnp.bfloat16)
        k_rot = rotate_half(rms_scale(k_heads, k_gain), cos_t[:, None, :], sin_t[:, None, :]).astype(jnp.bfloat16)
        k_wide = k_rot.astype(jnp.float32)
        v_wide = v_proj.reshape(SEQ_LEN, KV_HEADS, HEAD_DIM).astype(jnp.float32)
        q_blocks = q_rot.reshape(SEQ_LEN // Q_BLOCK, Q_BLOCK, KV_HEADS, GROUP_SIZE, HEAD_DIM)

        def one_block(block_args):
            q_block, block_start = block_args
            scores = jnp.einsum('qkgh,tkh->kgqt', q_block.astype(jnp.float32), k_wide) * (HEAD_DIM ** -0.5)
            query_index = block_start + jnp.arange(Q_BLOCK)
            allowed = query_index[:, None] >= key_index[None, :]
            scores = jnp.where(allowed, scores, -jnp.inf)
            attn_probs = jax.nn.softmax(scores, axis=-1).astype(jnp.bfloat16)
            mixed = jnp.einsum('kgqt,tkh->qkgh', attn_probs.astype(jnp.float32), v_wide)
            return mixed.astype(jnp.bfloat16)

        attn_out = lax.map(one_block, (q_blocks, block_starts)).reshape(SEQ_LEN, HEADS * HEAD_DIM)
        attn_sum = jnp.dot(attn_out, w_o, preferred_element_type=jnp.float32)
        return (x_f32 + attn_sum).astype(jnp.bfloat16)

    return lax.map(one_sequence, (x_resid, positions))
```

```python
import functools

import jax
import jax.numpy as jnp
from jax import lax
from jax.experimental import pallas as pl
from jax.experimental.pallas import tpu as pltpu
from jax.sharding import PartitionSpec as P

EPS = 1e-6
THETA = 1000000.0
MESH = pl.DeviceIdType.MESH
LOG2E = 1.4426950408889634


def body(x_in, pos_in, invf, ngain, qgain, kgain, wq_in, wk_in, wv_in, wo_in,
         out, wq_all, wk_all, wv_all, wo_all, xrel, yrel,
         xbuf, nbuf, obuf, wbuf, wobuf, qkvb, qs, ks, cosb, sinb, posbuf, posrel,
         a_send, a_recv, r_recv, w_own, w_fwd, w_sib, w_recv, w_loc, ld_sem, wo_sem):
    d_model = nbuf.shape[1]
    seq = nbuf.shape[0]
    n_seq = xbuf.shape[0]
    hd = ks.shape[1]
    n_heads = qs.shape[0]
    q_cols = n_heads * hd
    n_tp = wq_all.shape[0]
    chips = n_tp // 2
    piece = seq // n_tp
    dp_i = lax.axis_index('dp')
    me = lax.axis_index('tp')
    chip = me // 2
    core = me % 2

    def dev(dc, dk):
        return ((chip + dc + chips) % chips) * 2 + (core + dk) % 2

    def dev_abs(dc, k_abs):
        return ((chip + dc + chips) % chips) * 2 + k_abs

    sib = dev(0, 1)

    def rcopy(src, dst, ssem, rsem, target):
        return pltpu.make_async_remote_copy(src_ref=src, dst_ref=dst, send_sem=ssem, recv_sem=rsem,
                                            device_id=(dp_i, target), device_id_type=MESH)

    bar = pltpu.get_barrier_semaphore()
    near = [sib, dev_abs(1, 0), dev_abs(1, 1), dev_abs(-1, 0), dev_abs(-1, 1)]
    for t in near:
        pl.semaphore_signal(bar, inc=1, device_id=(dp_i, t), device_id_type=MESH)
    pl.semaphore_wait(bar, len(near))

    def rows(r):
        return pl.ds(pl.multiple_of(r * piece, piece), piece)

    def a2a_direct(a, src, dst, rel):
        far0, far1 = dev_abs(2, 0), dev_abs(2, 1)
        right, left = dev(1, 0), dev(-1, 0)
        return [
            rcopy(src(far0), rel(0), a_send.at[a, 0], r_recv.at[a, 0], right),
            rcopy(src(far1), rel(1), a_send.at[a, 1], r_recv.at[a, 1], left),
            rcopy(src(near[1]), dst(me, near[1]), a_send.at[a, 2], a_recv.at[a, me], near[1]),
            rcopy(src(near[3]), dst(me, near[3]), a_send.at[a, 3], a_recv.at[a, me], near[3]),
            rcopy(src(near[2]), dst(me, near[2]), a_send.at[a, 4], a_recv.at[a, me], near[2]),
            rcopy(src(near[4]), dst(me, near[4]), a_send.at[a, 5], a_recv.at[a, me], near[4]),
            rcopy(src(sib), dst(me, sib), a_send.at[a, 6], a_recv.at[a, me], sib),
        ]

    def a2a_local(a, src, dst):
        return pltpu.make_async_copy(src(me), dst(me, me), a_recv.at[a, me])

    def a2a_relay(a, dst, rel):
        s0, s1 = dev(-1, 0), dev(1, 0)
        return [
            rcopy(rel(0), dst(s0, near[1]), a_send.at[a, 7], a_recv.at[a, s0], near[1]),
            rcopy(rel(1), dst(s1, near[4]), a_send.at[a, 8], a_recv.at[a, s1], near[4]),
        ]

    def a2a_start(a, src, dst, rel):
        for c in a2a_direct(a, src, dst, rel):
            c.start()
        a2a_local(a, src, dst).start()

    def a2a_forward(a, dst, rel):
        fw = a2a_relay(a, dst, rel)
        for side in range(2):
            rcopy(rel(side), rel(side), a_send.at[a, 7 + side], r_recv.at[a, side], sib).wait_recv()
            fw[side].start()

    def a2a_wait(a, src, dst):
        a2a_local(a, src, dst).wait()
        for dc, dk in ((0, 1), (1, 0), (1, 1), (-1, 0), (-1, 1), (2, 0), (2, 1)):
            r = dev(dc, dk)
            ref = dst(r, me)
            rcopy(ref, ref, a_send.at[a, 0], a_recv.at[a, r], sib).wait_recv()

    def a2a_wait_sends(a, src, dst, rel):
        for c in a2a_direct(a, src, dst, rel) + a2a_relay(a, dst, rel):
            c.wait_send()

    def pos_src(r):
        return pos_in.at[r]

    def pos_dst(r, to):
        return posbuf.at[rows(r)]

    def pos_rel(side):
        return posrel.at[side]

    def x_fns(j):
        return (lambda r: x_in.at[r * n_seq + j],
                lambda r, to: xbuf.at[j, rows(r)],
                lambda side: xrel.at[j, side])

    def y_fns(j):
        return (lambda r: xbuf.at[j, rows(r)],
                lambda r, to: out.at[r * n_seq + j],
                lambda side: yrel.at[j, side])

    def set_x(j):
        return 1 + j

    def set_y(j):
        return 1 + n_seq + j

    w_in = (wq_in, wk_in, wv_in, wo_in)
    w_all = (wq_all, wk_all, wv_all, wo_all)

    def w_send_own(i, which, target):
        return rcopy(w_in[i], w_all[i].at[me], w_own.at[which, i], w_recv.at[me, i], target)

    def w_wait(i, r):
        ref = w_all[i].at[r]
        rcopy(ref, ref, w_own.at[0, 0], w_recv.at[r, i], sib).wait_recv()

    def w_to_sib(i, r, slot):
        return rcopy(w_all[i].at[r], w_all[i].at[r], w_sib.at[slot, i], w_recv.at[r, i], sib)

    def w_onward(i, r, target):
        return rcopy(w_all[i].at[r], w_all[i].at[r], w_fwd.at[i], w_recv.at[r, i], target)

    left, right, far = dev(-1, 0), dev(1, 0), dev(2, 0)
    Q, K, V, O = range(4)

    a2a_start(0, pos_src, pos_dst, pos_rel)
    a2a_start(set_x(0), *x_fns(0))
    for i in range(4):
        w_send_own(i, 0, sib).start()
    w_local = [pltpu.make_async_copy(w_in[i], w_all[i].at[me], w_loc.at[i]) for i in range(4)]
    a2a_forward(0, pos_dst, pos_rel)
    a2a_forward(set_x(0), *x_fns(0)[1:])
    for i in (Q, K, O, V):
        w_send_own(i, 1, right).start()
    for i in (O, V, Q, K):
        w_send_own(i, 2, left).start()
    for c in w_local:
        c.start()
    a2a_wait(0, pos_src, pos_dst)

    lane = lax.broadcasted_iota(jnp.int32, (piece, hd), 1)

    def table_step(r, _):
        rs = rows(r)
        for j in range(n_seq):
            ang = posbuf[rs, j:j + 1] * invf[...]
            cosb[j, rs, :] = jnp.cos(ang)
            sn = jnp.sin(ang)
            sinb[j, rs, :] = jnp.where(lane < hd // 2, -sn, sn)
        return 0

    lax.fori_loop(0, n_tp, table_step, 0)

    def gid(s):
        m = s // 2
        return ((chip + (3 * m * (m + 1) // 2)) % chips) * 2 + (core + s) % 2

    cols = ((Q, 0, q_cols), (K, q_cols, hd), (V, q_cols + hd, hd))

    def load_w(g, slot):
        return [pltpu.make_async_copy(w_all[i].at[g], wbuf.at[slot, :, c0:c0 + cn], ld_sem.at[slot, i])
                for i, c0, cn in cols]

    def load_own(slot):
        return [pltpu.make_async_copy(w_in[i], wbuf.at[slot, :, c0:c0 + cn], ld_sem.at[slot, i])
                for i, c0, cn in cols]

    nt_cols = wobuf.shape[3]
    n_nt = d_model // nt_cols

    def load_wo(nt, slot):
        return pltpu.make_async_copy(wo_all.at[:, :, pl.ds(pl.multiple_of(nt * nt_cols, nt_cols), nt_cols)],
                                     wobuf.at[slot], wo_sem.at[slot])

    scale2 = (hd ** -0.5) * LOG2E
    blk = 128
    n_blk = seq // blk
    rmod = lax.broadcasted_iota(jnp.int32, (n_heads, blk, blk), 1)
    cmod = lax.broadcasted_iota(jnp.int32, (n_heads, blk, blk), 2)
    tri = (rmod >= cmod).reshape(n_heads * blk, blk)

    def norm_rope(u, gain, cs, sn):
        u = u.astype(jnp.float32)
        ms = jnp.mean(u * u, axis=-1, keepdims=True)
        w = u * lax.rsqrt(ms + EPS) * gain
        return (w * cs + pltpu.roll(w, hd // 2, 1) * sn).astype(jnp.bfloat16)

    def unit(j, g, slot):
        qkvb[...] = jnp.dot(nbuf[...], wbuf[slot], preferred_element_type=jnp.float32).astype(jnp.bfloat16)

        def rope_step(b, _):
            rs = pl.ds(pl.multiple_of(b * 64, 64), 64)
            cs, sn = cosb[j, rs, :], sinb[j, rs, :]
            for h in range(n_heads):
                qs[h, rs, :] = norm_rope(qkvb[rs, h * hd:(h + 1) * hd], qgain[...], cs, sn)
            ks[rs, :] = norm_rope(qkvb[rs, q_cols:q_cols + hd], kgain[...], cs, sn)
            return 0

        lax.fori_loop(0, seq // 64, rope_step, 0)
        ocol = pl.multiple_of(g * q_cols, q_cols)
        for i in range(n_blk):
            kl = (i + 1) * blk
            lhs = qs[:, i * blk:kl, :].reshape(n_heads * blk, hd)
            s = lax.dot_general(lhs, ks[:kl, :], (((1,), (1,)), ((), ())), preferred_element_type=jnp.float32)
            diag = jnp.where(tri, s[:, i * blk:kl], -jnp.inf)
            s = diag if i == 0 else jnp.concatenate([s[:, :i * blk], diag], axis=1)
            peak = jnp.max(s, axis=-1, keepdims=True)
            e = jnp.exp2((s - peak) * scale2)
            inv = 1.0 / jnp.sum(e, axis=-1, keepdims=True)
            p = (e * inv).astype(jnp.bfloat16)
            o = jnp.dot(p, qkvb[:kl, q_cols + hd:q_cols + 2 * hd], preferred_element_type=jnp.float32)
            o = o.astype(jnp.bfloat16)
            for h in range(n_heads):
                obuf[i * blk:kl, pl.ds(pl.multiple_of(ocol + h * hd, hd), hd)] = o[h * blk:(h + 1) * blk]

    n_grp = n_tp
    last = n_seq * n_grp - 1

    def comm_first(s):
        @pl.when(s == 1)
        def _():
            for i in range(4):
                w_wait(i, sib)

        @pl.when(s == 2)
        def _():
            for i in (Q, K):
                w_wait(i, left)
                w_onward(i, left, right).start()
                w_to_sib(i, left, 0).start()
                oi = {Q: O, K: V}[i]
                w_wait(oi, right)
                w_onward(oi, right, left).start()
                w_to_sib(oi, right, 1).start()
            a2a_start(set_x(1), *x_fns(1))
            for i in (O, V):
                w_wait(i, left)
                w_to_sib(i, left, 0).start()
                oi = {O: Q, V: K}[i]
                w_wait(oi, right)
                w_to_sib(oi, right, 1).start()
            for c in w_local:
                c.wait()

        @pl.when(s == 3)
        def _():
            for i in range(4):
                w_wait(i, dev(-1, 1))

        @pl.when(s == 5)
        def _():
            for i in range(4):
                w_wait(i, dev(1, 1))

        @pl.when(s == 6)
        def _():
            for i in (Q, O, K, V):
                w_wait(i, far)
                w_to_sib(i, far, 2).start()

        @pl.when(s == 7)
        def _():
            for i in range(4):
                w_wait(i, dev(2, 1))

    def seq_step(j, _):
        a2a_wait(set_x(j), *x_fns(j)[:2])

        def n_step(r, _):
            rs = rows(r)
            xv = xbuf[j, rs, :].astype(jnp.float32)
            ms = jnp.mean(xv * xv, axis=-1, keepdims=True)
            nbuf[rs, :] = (xv * lax.rsqrt(ms + EPS) * ngain[...]).astype(jnp.bfloat16)
            return 0

        lax.fori_loop(0, n_tp, n_step, 0)

        def grp_step(s, _):
            t = j * n_grp + s
            slot = t % 2

            @pl.when(j == 0)
            def _():
                comm_first(s)

                @pl.when(s == 0)
                def _():
                    for c in load_own(slot):
                        c.start()

                @pl.when(s > 0)
                def _():
                    for c in load_w(gid(s), slot):
                        c.start()

            @pl.when(jnp.logical_and(j > 0, s == 2))
            def _():
                a2a_forward(set_y(j - 1), *y_fns(j - 1)[1:])

            for c in load_w(gid(s), slot):
                c.wait()

            @pl.when(jnp.logical_and(t >= n_grp - 1, t < last))
            def _():
                for c in load_w(gid((s + 1) % n_grp), 1 - slot):
                    c.start()

            @pl.when(s == n_grp - 1)
            def _():
                load_wo(0, 0).start()

                @pl.when(j + 1 < n_seq)
                def _():
                    a2a_forward(set_x(j + 1), *x_fns(j + 1)[1:])

                @pl.when(j + 2 < n_seq)
                def _():
                    a2a_start(set_x(j + 2), *x_fns(j + 2))

            unit(j, gid(s), slot)
            return 0

        lax.fori_loop(0, n_grp, grp_step, 0)

        def out_step(nt, _):
            ws = nt % 2
            load_wo(nt, ws).wait()

            @pl.when(nt + 1 < n_nt)
            def _():
                load_wo(nt + 1, 1 - ws).start()

            cs = pl.ds(pl.multiple_of(nt * nt_cols, nt_cols), nt_cols)
            acc = jnp.dot(obuf[...], wobuf[ws].reshape(n_tp * q_cols, nt_cols), preferred_element_type=jnp.float32)
            xbuf[j, :, cs] = (xbuf[j, :, cs].astype(jnp.float32) + acc).astype(jnp.bfloat16)
            return 0

        lax.fori_loop(0, n_nt, out_step, 0)
        a2a_start(set_y(j), *y_fns(j))
        return 0

    lax.fori_loop(0, n_seq, seq_step, 0)

    a2a_forward(set_y(n_seq - 1), *y_fns(n_seq - 1)[1:])
    for i in range(4):
        w_send_own(i, 0, sib).wait_send()
        w_send_own(i, 1, right).wait_send()
        w_send_own(i, 2, left).wait_send()
    for i in (Q, K):
        w_onward(i, left, right).wait_send()
    for i in (O, V):
        w_onward(i, right, left).wait_send()
    for i in range(4):
        for slot, r in enumerate((left, right, far)):
            w_to_sib(i, r, slot).wait_send()
    a2a_wait_sends(0, pos_src, pos_dst, pos_rel)

    def end_step(j, _):
        a2a_wait_sends(set_x(j), *x_fns(j))
        a2a_wait(set_y(j), *y_fns(j)[:2])
        a2a_wait_sends(set_y(j), *y_fns(j))
        return 0

    lax.fori_loop(0, n_seq, end_step, 0)


def solution(mesh):
    n_tp = mesh.shape['tp']

    def local_block(x_loc, pos_loc, norm_gain, w_q, w_k, w_v, q_gain, k_gain, w_o):
        batch, piece, d_model = x_loc.shape
        hd = q_gain.shape[0]
        q_cols = w_q.shape[1]
        n_heads = q_cols // hd
        n_seq = batch // n_tp
        seq = piece * n_tp
        f32, bf16 = jnp.float32, jnp.bfloat16
        pos = pos_loc.astype(f32).reshape(n_tp, n_seq, piece).transpose(0, 2, 1)
        pos = jnp.pad(pos, ((0, 0), (0, 0), (0, hd - n_seq)))
        inv_freq = THETA ** (-(jnp.arange(hd // 2, dtype=f32) * (2.0 / hd)))
        invf = jnp.concatenate([inv_freq, inv_freq])[None, :]
        any_spec = pl.BlockSpec(memory_space=pl.ANY)
        vmem = pl.BlockSpec(memory_space=pltpu.VMEM)
        nt_cols = 512
        dma = pltpu.SemaphoreType.DMA
        n_sets = 1 + 2 * n_seq
        res = pl.pallas_call(
            body,
            name='attn_block',
            out_shape=[
                jax.ShapeDtypeStruct((batch, piece, d_model), bf16),
                jax.ShapeDtypeStruct((n_tp,) + w_q.shape, bf16),
                jax.ShapeDtypeStruct((n_tp,) + w_k.shape, bf16),
                jax.ShapeDtypeStruct((n_tp,) + w_v.shape, bf16),
                jax.ShapeDtypeStruct((n_tp,) + w_o.shape, bf16),
                jax.ShapeDtypeStruct((n_seq, 2, piece, d_model), bf16),
                jax.ShapeDtypeStruct((n_seq, 2, piece, d_model), bf16),
            ],
            in_specs=[any_spec, any_spec, vmem, vmem, vmem, vmem, any_spec, any_spec, any_spec, any_spec],
            out_specs=[any_spec] * 7,
            scratch_shapes=[
                pltpu.VMEM((n_seq, seq, d_model), bf16),
                pltpu.VMEM((seq, d_model), bf16),
                pltpu.VMEM((seq, n_tp * q_cols), bf16),
                pltpu.VMEM((2, d_model, q_cols + 2 * hd), bf16),
                pltpu.VMEM((2, n_tp, q_cols, nt_cols), bf16),
                pltpu.VMEM((seq, q_cols + 2 * hd), bf16),
                pltpu.VMEM((n_heads, seq, hd), bf16),
                pltpu.VMEM((seq, hd), bf16),
                pltpu.VMEM((n_seq, seq, hd), f32),
                pltpu.VMEM((n_seq, seq, hd), f32),
                pltpu.VMEM((seq, hd), f32),
                pltpu.VMEM((2, piece, hd), f32),
                dma((n_sets, 9)),
                dma((n_sets, n_tp)),
                dma((n_sets, 2)),
                dma((3, 4)),
                dma((4,)),
                dma((3, 4)),
                dma((n_tp, 4)),
                dma((4,)),
                dma((2, 3)),
                dma((2,)),
            ],
            compiler_params=pltpu.CompilerParams(
                collective_id=0, has_side_effects=True, vmem_limit_bytes=62 * 1024 * 1024),
        )(x_loc, pos, invf, norm_gain.astype(f32)[None, :], q_gain.astype(f32)[None, :],
          k_gain.astype(f32)[None, :], w_q, w_k, w_v, w_o)
        return res[0]

    return jax.shard_map(
        local_block, mesh=mesh,
        in_specs=(P('dp', 'tp', None), P('dp', 'tp'), P(None), P(None, 'tp'), P(None, 'tp'), P(None, 'tp'),
                  P(None), P(None), P('tp', None)),
        out_specs=P('dp', 'tp', None), check_vma=False)
```

```python
import jax
import jax.numpy as jnp
from jax import lax
from jax.experimental import pallas as pl
from jax.experimental.pallas import tpu as pltpu
from jax.sharding import PartitionSpec as P

EPS = 1e-6
THETA = 1000000.0
MESH = pl.DeviceIdType.MESH
LOG2E = 1.4426950408889634


SHARE = True


def body(x_in, pos_in, invf, ngain, qgain, kgain, wt_in, wo_in,
         out, wt_all, wo_all,
         xbuf, nbuf, obuf, wtb, wobuf, qkvt, qt, ks, vt, qcos, qsin, kcos, ksin, posbuf,
         a_send, a_recv, w_own, w_fwd, w_sib, w_pair, w_recv, w_loc, ld_sem, wo_sem):
    d_model = nbuf.shape[1]
    seq = nbuf.shape[0]
    n_seq = xbuf.shape[0]
    hd = ks.shape[1]
    q_cols = qt.shape[0]
    n_heads = q_cols // hd
    n_tp = wt_all.shape[0]
    n_dp = lax.axis_size('dp')
    share = SHARE and n_dp % 2 == 0
    chips = n_tp // 2
    piece = seq // n_tp
    dp_i = lax.axis_index('dp')
    me = lax.axis_index('tp')
    chip = me // 2
    core = me % 2

    def dev(dc, dk):
        return ((chip + dc + chips) % chips) * 2 + (core + dk) % 2

    sib = dev(0, 1)

    def rcopy(src, dst, ssem, rsem, target):
        return pltpu.make_async_remote_copy(src_ref=src, dst_ref=dst, send_sem=ssem, recv_sem=rsem,
                                            device_id=(dp_i, target), device_id_type=MESH)

    bar = pltpu.get_barrier_semaphore()
    near = [dev(dc, dk) for dc in (-1, 1, 2) for dk in (0, 1)] + [sib]
    for t in near:
        pl.semaphore_signal(bar, inc=1, device_id=(dp_i, t), device_id_type=MESH)
    par = dp_i % 2
    mate = dp_i + 1 - 2 * par
    if share:
        pl.semaphore_signal(bar, inc=1, device_id=(mate, me), device_id_type=MESH)
    pl.semaphore_wait(bar, len(near) + (1 if share else 0))

    def rows(r):
        return pl.ds(pl.multiple_of(r * piece, piece), piece)

    others = ((2, 0), (2, 1), (1, 0), (1, 1), (-1, 0), (-1, 1), (0, 1))

    def a2a_direct(a, src, dst):
        return [rcopy(src(dev(*o)), dst(me, dev(*o)), a_send.at[a, n], a_recv.at[a, me], dev(*o))
                for n, o in enumerate(others)]

    def a2a_local(a, src, dst):
        return pltpu.make_async_copy(src(me), dst(me, me), a_recv.at[a, me])

    def a2a_start(a, src, dst):
        for c in a2a_direct(a, src, dst):
            c.start()
        a2a_local(a, src, dst).start()

    def a2a_wait(a, src, dst):
        a2a_local(a, src, dst).wait()
        for o in others:
            r = dev(*o)
            ref = dst(r, me)
            rcopy(ref, ref, a_send.at[a, 0], a_recv.at[a, r], sib).wait_recv()

    def a2a_wait_sends(a, src, dst):
        for c in a2a_direct(a, src, dst):
            c.wait_send()

    def pos_src(r):
        return pos_in.at[r]

    def pos_dst(r, to):
        return posbuf.at[rows(r)]

    def x_fns(j):
        return (lambda r: x_in.at[r * n_seq + j],
                lambda r, to: xbuf.at[j, rows(r)])

    def y_fns(j):
        return (lambda r: xbuf.at[j, rows(r)],
                lambda r, to: out.at[r * n_seq + j])

    def set_x(j):
        return 1 + j

    def set_y(j):
        return 1 + n_seq + j

    Q, KV, O = range(3)

    def half(i, h):
        n = (q_cols // 2, hd, q_cols // 2)[i]
        return pl.ds(pl.multiple_of(h * n + (q_cols if i == KV else 0), n), n)

    def win(i, h):
        return (wo_in if i == O else wt_in).at[half(i, h)]

    def wref(i, h, r):
        return (wo_all if i == O else wt_all).at[r, half(i, h)]

    def w_send_own(p, which, target):
        i, h = p
        return rcopy(win(i, h), wref(i, h, me), w_own.at[which, 2 * i + h], w_recv.at[me, 2 * i + h],
                     target)

    def w_wait(p, r):
        i, h = p
        ref = wref(i, h, r)
        rcopy(ref, ref, w_own.at[0, 0], w_recv.at[r, 2 * i + h], sib).wait_recv()

    def w_to_sib(p, r, slot):
        i, h = p
        return rcopy(wref(i, h, r), wref(i, h, r), w_sib.at[slot, 2 * i + h], w_recv.at[r, 2 * i + h], sib)

    def w_onward(p, r, target):
        i, h = p
        return rcopy(wref(i, h, r), wref(i, h, r), w_fwd.at[2 * i + h], w_recv.at[r, 2 * i + h], target)

    def w_to_mate(p, r, slot):
        i, h = p
        return pltpu.make_async_remote_copy(
            src_ref=wref(i, h, r), dst_ref=wref(i, h, r), send_sem=w_pair.at[slot, 2 * i + h],
            recv_sem=w_recv.at[r, 2 * i + h], device_id=(mate, me), device_id_type=MESH)

    left, right, far = dev(-1, 0), dev(1, 0), dev(2, 0)
    L, R, F = (left, 0), (right, 1), (far, 2)
    every = [(i, h) for i in range(3) for h in range(2)]
    if share:
        first, from_mate = [(Q, par), (KV, par)], [(Q, 1 - par), (KV, 1 - par)]
    else:
        first, from_mate = [(Q, 0), (KV, 0), (Q, 1), (KV, 1)], []
    later = [(O, 0), (O, 1)]

    def got(p, src, onward=None):
        r, slot = src
        w_wait(p, r)
        if onward is not None:
            w_onward(p, r, onward).start()
        if share and p[0] != O:
            w_to_mate(p, r, slot).start()
        w_to_sib(p, r, slot).start()

    def got_mate(p, src):
        r, slot = src
        w_wait(p, r)
        w_to_sib(p, r, slot).start()

    a2a_start(0, pos_src, pos_dst)
    for p in first:
        w_send_own(p, 1, right).start()
        w_send_own(p, 2, left).start()
    for p in every:
        w_send_own(p, 0, sib).start()
    a2a_start(set_x(0), *x_fns(0))
    for p in later:
        w_send_own(p, 2, left).start()
    w_local = [pltpu.make_async_copy(wt_in, wt_all.at[me], w_loc.at[0]),
               pltpu.make_async_copy(wo_in, wo_all.at[me], w_loc.at[1])]
    for c in w_local:
        c.start()
    a2a_wait(0, pos_src, pos_dst)

    blk = 128
    lane = lax.broadcasted_iota(jnp.int32, (blk, hd), 1)

    def table_step(b, _):
        rs = pl.ds(pl.multiple_of(b * blk, blk), blk)
        for j in range(n_seq):
            ang = posbuf[rs, j:j + 1] * invf[...]
            cs = jnp.cos(ang)
            sn = jnp.sin(ang)
            sn = jnp.where(lane < hd // 2, -sn, sn)
            qcos[j, :, rs] = (cs * qgain[0:1, :]).T
            qsin[j, :, rs] = (sn * qgain[1:2, :]).T
            kcos[j, :, rs] = (cs * kgain[0:1, :]).T
            ksin[j, :, rs] = (sn * kgain[1:2, :]).T
        return 0

    lax.fori_loop(0, seq // blk, table_step, 0)

    for p in first:
        got(p, L, right)
        got(p, R)
    a2a_start(set_x(1), *x_fns(1))
    for p in later:
        w_send_own(p, 1, right).start()

    def wait_all(arrays, r):
        for i in arrays:
            for h in range(2):
                w_wait((i, h), r)

    def stage(s):
        @pl.when(s == 2)
        def _():
            for p in from_mate[:1]:
                got_mate(p, L)
                got_mate(p, R)
            for p in from_mate[1:]:
                got_mate(p, L)

        @pl.when(s == 3)
        def _():
            wait_all((Q, KV), dev(-1, 1))
            got(first[0], F)

        @pl.when(s == 4)
        def _():
            for p in from_mate[1:]:
                got_mate(p, R)
            for p in first[1:]:
                got(p, F)

        @pl.when(s == 5)
        def _():
            wait_all((Q, KV), dev(1, 1))

        @pl.when(s == 6)
        def _():
            for p in later:
                got(p, R, left)
            a2a_start(set_x(2), *x_fns(2))
            a2a_start(set_x(3), *x_fns(3))
            for p in from_mate:
                got_mate(p, F)

        @pl.when(s == 7)
        def _():
            wait_all((Q, KV), dev(2, 1))
            for c in w_local:
                c.wait()

    def gid(s):
        m = s // 2
        return ((chip + 3 * m * (m + 1) // 2) % chips) * 2 + (core + s) % 2

    def load_w(g, slot):
        return [pltpu.make_async_copy(wt_all.at[g], wtb.at[slot], ld_sem.at[slot])]

    nt_cols = wobuf.shape[3]
    n_nt = d_model // nt_cols

    def load_wo(nt, slot):
        return pltpu.make_async_copy(wo_all.at[:, :, pl.ds(pl.multiple_of(nt * nt_cols, nt_cols), nt_cols)],
                                     wobuf.at[slot], wo_sem.at[slot])

    scale2 = (hd ** -0.5) * LOG2E
    n_blk = seq // blk
    key_i = lax.broadcasted_iota(jnp.int32, (blk, 2 * blk), 0)
    qry_i = lax.broadcasted_iota(jnp.int32, (blk, 2 * blk), 1) % blk
    tri = key_i <= qry_i

    def norm_rope(row, ls, cos, sin):
        mid = hd // 2
        u1 = qkvt[row:row + mid, ls].astype(jnp.float32)
        u2 = qkvt[row + mid:row + hd, ls].astype(jnp.float32)
        r = lax.rsqrt(jnp.sum(u1 * u1 + u2 * u2, axis=0, keepdims=True) * (1.0 / hd) + EPS)
        return ((u1 * cos[:mid] + u2 * sin[:mid]) * r, (u2 * cos[mid:] + u1 * sin[mid:]) * r)

    def project(slot):
        qkvt[...] = lax.dot_general(wtb[slot], nbuf[...], (((1,), (1,)), ((), ())),
                                    preferred_element_type=jnp.float32).astype(jnp.bfloat16)

    def rope(j):
        mid = hd // 2
        for b in range(n_blk):
            ls = slice(b * blk, (b + 1) * blk)
            o1, o2 = norm_rope(q_cols, ls, kcos[j, :, ls], ksin[j, :, ls])
            ks[ls, :] = jnp.concatenate([o1, o2], axis=0).T.astype(jnp.bfloat16)
            cos, sin = qcos[j, :, ls], qsin[j, :, ls]
            for h in range(n_heads):
                o1, o2 = norm_rope(h * hd, ls, cos, sin)
                qt[h * hd:h * hd + mid, ls] = o1.astype(jnp.bfloat16)
                qt[h * hd + mid:(h + 1) * hd, ls] = o2.astype(jnp.bfloat16)
        vt[...] = qkvt[q_cols + hd:, :]

    def attend(j, g):
        oj = j % 2
        ocol = pl.multiple_of(g * q_cols, q_cols)
        for i in range(n_blk):
            kl = (i + 1) * blk
            for h in range(0, n_heads, 2):
                q2 = jnp.concatenate([qt[(h + k) * hd:(h + k + 1) * hd, i * blk:kl] for k in range(2)], axis=1)
                s = jnp.dot(ks[:kl, :], q2, preferred_element_type=jnp.float32)
                diag = jnp.where(tri, s[i * blk:, :], -jnp.inf)
                s = diag if i == 0 else jnp.concatenate([s[:i * blk, :], diag], axis=0)
                peak = jnp.max(s, axis=0, keepdims=True)
                e = jnp.exp2((s - peak) * scale2)
                inv = 1.0 / jnp.sum(e, axis=0, keepdims=True)
                p = (e * inv).astype(jnp.bfloat16)
                o = jnp.dot(vt[:, :kl], p, preferred_element_type=jnp.float32)
                for k in range(2):
                    obuf[oj, i * blk:kl, pl.ds(pl.multiple_of(ocol + (h + k) * hd, hd), hd)] = (
                        o[:, k * blk:(k + 1) * blk].T.astype(jnp.bfloat16))

    n_grp = n_tp
    n_units = n_seq * n_grp

    def normalise(j):
        a2a_wait(set_x(j), *x_fns(j))

        def n_step(r, _):
            rs = rows(r)
            xv = xbuf[j, rs, :].astype(jnp.float32)
            ms = jnp.mean(xv * xv, axis=-1, keepdims=True)
            nbuf[rs, :] = (xv * lax.rsqrt(ms + EPS) * ngain[...]).astype(jnp.bfloat16)
            return 0

        lax.fori_loop(0, n_tp, n_step, 0)

    def out_proj(j):
        def out_step(nt, _):
            ws = nt % 2
            load_wo(nt, ws).wait()

            @pl.when(nt + 1 < n_nt)
            def _():
                load_wo(nt + 1, 1 - ws).start()

            cs = pl.ds(pl.multiple_of(nt * nt_cols, nt_cols), nt_cols)
            acc = jnp.dot(obuf[j % 2], wobuf[ws].reshape(n_tp * q_cols, nt_cols), preferred_element_type=jnp.float32)
            xbuf[j, :, cs] = (xbuf[j, :, cs].astype(jnp.float32) + acc).astype(jnp.bfloat16)
            return 0

        load_wo(0, 0).start()
        lax.fori_loop(0, n_nt, out_step, 0)
        a2a_start(set_y(j), *y_fns(j))

    own_load = pltpu.make_async_copy(wt_in, wtb.at[0], ld_sem.at[0])
    own_load.start()
    wait_all((Q, KV), sib)
    for c in load_w(gid(1), 1):
        c.start()
    normalise(0)
    own_load.wait()
    project(0)

    def step(t, _):
        j, s = t // n_grp, t % n_grp
        u = t + 1

        @pl.when(j == 0)
        def _():
            stage(s + 2)

        @pl.when(jnp.logical_and(j == 1, s == 2))
        def _():
            got(later[0], L)
            got(later[0], F)

        @pl.when(jnp.logical_and(j == 1, s == 5))
        def _():
            got(later[1], L)
            got(later[1], F)

        @pl.when(u + 1 < n_units)
        def _():
            for c in load_w(gid((u + 1) % n_grp), (u + 1) % 2):
                c.start()

        @pl.when(u < n_units)
        def _():
            for c in load_w(gid(u % n_grp), u % 2):
                c.wait()

        @pl.when(s == n_grp - 1)
        def _():
            @pl.when(u < n_units)
            def _():
                normalise(j + 1)

        rope(j)
        attend(j, gid(s))
        project(u % 2)

        @pl.when(jnp.logical_and(j == 1, s == n_grp - 1))
        def _():
            wait_all((O,), sib)
            for dc in (-1, 1, 2):
                wait_all((O,), dev(dc, 1))

        @pl.when(jnp.logical_and(j > 0, s == n_grp - 1))
        def _():
            def turn(jj, _):
                out_proj(jj)
                return 0

            lax.fori_loop(j * ((j + 2) // 4), j + 1, turn, 0)

        return 0

    lax.fori_loop(0, n_units, step, 0)

    for p in every:
        w_send_own(p, 0, sib).wait_send()
        for slot, r in enumerate((left, right, far)):
            w_to_sib(p, r, slot).wait_send()
    for p in first + later:
        w_send_own(p, 1, right).wait_send()
        w_send_own(p, 2, left).wait_send()
    for p in first:
        w_onward(p, left, right).wait_send()
    for p in later:
        w_onward(p, right, left).wait_send()
    if share:
        for p in first:
            for slot, r in enumerate((left, right, far)):
                w_to_mate(p, r, slot).wait_send()
    a2a_wait_sends(0, pos_src, pos_dst)

    def end_step(j, _):
        a2a_wait_sends(set_x(j), *x_fns(j))
        a2a_wait(set_y(j), *y_fns(j))
        a2a_wait_sends(set_y(j), *y_fns(j))
        return 0

    lax.fori_loop(0, n_seq, end_step, 0)


def gain_rows(gain):
    g = gain.astype(jnp.float32)
    return jnp.stack([g, jnp.roll(g, g.shape[0] // 2)])


def solution(mesh):
    n_tp = mesh.shape['tp']

    def local_block(x_loc, pos_loc, norm_gain, w_q, w_k, w_v, q_gain, k_gain, w_o):
        batch, piece, d_model = x_loc.shape
        hd = q_gain.shape[0]
        q_cols = w_q.shape[1]
        n_seq = batch // n_tp
        seq = piece * n_tp
        f32, bf16 = jnp.float32, jnp.bfloat16
        pos = pos_loc.astype(f32).reshape(n_tp, n_seq, piece).transpose(0, 2, 1)
        pos = jnp.pad(pos, ((0, 0), (0, 0), (0, hd - n_seq)))
        inv_freq = THETA ** (-(jnp.arange(hd // 2, dtype=f32) * (2.0 / hd)))
        invf = jnp.concatenate([inv_freq, inv_freq])[None, :]
        any_spec = pl.BlockSpec(memory_space=pl.ANY)
        vmem = pl.BlockSpec(memory_space=pltpu.VMEM)
        nt_cols = 512
        dma = pltpu.SemaphoreType.DMA
        n_sets = 1 + 2 * n_seq
        w_t = jnp.concatenate([w_q, w_k, w_v], axis=1).T
        res = pl.pallas_call(
            body,
            name='attn_block',
            out_shape=[
                jax.ShapeDtypeStruct((batch, piece, d_model), bf16),
                jax.ShapeDtypeStruct((n_tp,) + w_t.shape, bf16),
                jax.ShapeDtypeStruct((n_tp,) + w_o.shape, bf16),
            ],
            in_specs=[any_spec, any_spec, vmem, vmem, vmem, vmem, any_spec, any_spec],
            out_specs=[any_spec] * 3,
            scratch_shapes=[
                pltpu.VMEM((n_seq, seq, d_model), bf16),
                pltpu.VMEM((seq, d_model), bf16),
                pltpu.VMEM((2, seq, n_tp * q_cols), bf16),
                pltpu.VMEM((2,) + w_t.shape, bf16),
                pltpu.VMEM((2, n_tp, q_cols, nt_cols), bf16),
                pltpu.VMEM((q_cols + 2 * hd, seq), bf16),
                pltpu.VMEM((q_cols, seq), bf16),
                pltpu.VMEM((seq, hd), bf16),
                pltpu.VMEM((hd, seq), bf16),
                pltpu.VMEM((n_seq, hd, seq), f32),
                pltpu.VMEM((n_seq, hd, seq), f32),
                pltpu.VMEM((n_seq, hd, seq), f32),
                pltpu.VMEM((n_seq, hd, seq), f32),
                pltpu.VMEM((seq, hd), f32),
                dma((n_sets, n_tp - 1)),
                dma((n_sets, n_tp)),
                dma((3, 6)),
                dma((6,)),
                dma((3, 6)),
                dma((3, 6)),
                dma((n_tp, 6)),
                dma((2,)),
                dma((2,)),
                dma((2,)),
            ],
            compiler_params=pltpu.CompilerParams(
                collective_id=0, has_side_effects=True, vmem_limit_bytes=62 * 1024 * 1024),
        )(x_loc, pos, invf, norm_gain.astype(f32)[None, :], gain_rows(q_gain), gain_rows(k_gain), w_t, w_o)
        return res[0]

    return jax.shard_map(
        local_block, mesh=mesh,
        in_specs=(P('dp', 'tp', None), P('dp', 'tp'), P(None), P(None, 'tp'), P(None, 'tp'), P(None, 'tp'),
                  P(None), P(None), P('tp', None)),
        out_specs=P('dp', 'tp', None), check_vma=False)
```

```python
import jax
import jax.numpy as jnp
from jax import lax
from jax.experimental import pallas as pl
from jax.experimental.pallas import tpu as pltpu
from jax.sharding import PartitionSpec as P

EPS = 1e-6
THETA = 1000000.0
MESH = pl.DeviceIdType.MESH
LOG2E = 1.4426950408889634


SHARE = True


def body(x_in, pos_in, invf, ngain, qgain, kgain, wt_in, wo_in,
         out, wt_all, wo_all,
         xbuf, nbuf, obuf, wtb, wobuf, qkvt, qt, ks, vt, qcos, qsin, kcos, ksin, posbuf,
         a_send, a_recv, w_own, w_fwd, w_sib, w_pair, w_recv, w_loc, ld_sem, wo_sem):
    d_model = nbuf.shape[1]
    seq = nbuf.shape[0]
    n_seq = xbuf.shape[0]
    hd = ks.shape[1]
    q_cols = qt.shape[0]
    n_heads = q_cols // hd
    n_tp = wt_all.shape[0]
    n_dp = lax.axis_size('dp')
    share = SHARE and n_dp % 2 == 0
    chips = n_tp // 2
    piece = seq // n_tp
    dp_i = lax.axis_index('dp')
    me = lax.axis_index('tp')
    chip = me // 2
    core = me % 2

    def dev(dc, dk):
        return ((chip + dc + chips) % chips) * 2 + (core + dk) % 2

    sib = dev(0, 1)

    def rcopy(src, dst, ssem, rsem, target):
        return pltpu.make_async_remote_copy(src_ref=src, dst_ref=dst, send_sem=ssem, recv_sem=rsem,
                                            device_id=(dp_i, target), device_id_type=MESH)

    bar = pltpu.get_barrier_semaphore()
    near = [dev(dc, dk) for dc in (-1, 1, 2) for dk in (0, 1)] + [sib]
    for t in near:
        pl.semaphore_signal(bar, inc=1, device_id=(dp_i, t), device_id_type=MESH)
    par = dp_i % 2
    mate = dp_i + 1 - 2 * par
    if share:
        pl.semaphore_signal(bar, inc=1, device_id=(mate, me), device_id_type=MESH)
    pl.semaphore_wait(bar, len(near) + (1 if share else 0))

    def rows(r):
        return pl.ds(pl.multiple_of(r * piece, piece), piece)

    others = ((2, 0), (2, 1), (1, 0), (1, 1), (-1, 0), (-1, 1), (0, 1))

    def a2a_direct(a, src, dst):
        return [rcopy(src(dev(*o)), dst(me, dev(*o)), a_send.at[a, n], a_recv.at[a, me], dev(*o))
                for n, o in enumerate(others)]

    def a2a_local(a, src, dst):
        return pltpu.make_async_copy(src(me), dst(me, me), a_recv.at[a, me])

    def a2a_start(a, src, dst):
        for c in a2a_direct(a, src, dst):
            c.start()
        a2a_local(a, src, dst).start()

    def a2a_wait(a, src, dst):
        a2a_local(a, src, dst).wait()
        for o in others:
            r = dev(*o)
            ref = dst(r, me)
            rcopy(ref, ref, a_send.at[a, 0], a_recv.at[a, r], sib).wait_recv()

    def a2a_wait_sends(a, src, dst):
        for c in a2a_direct(a, src, dst):
            c.wait_send()

    def pos_src(r):
        return pos_in.at[r]

    def pos_dst(r, to):
        return posbuf.at[rows(r)]

    def x_fns(j):
        return (lambda r: x_in.at[r * n_seq + j],
                lambda r, to: xbuf.at[j, rows(r)])

    def y_fns(j):
        return (lambda r: xbuf.at[j, rows(r)],
                lambda r, to: out.at[r * n_seq + j])

    def set_x(j):
        return 1 + j

    def set_y(j):
        return 1 + n_seq + j

    Q, KV, O = range(3)

    n_cut = (2, 2, 4)
    base = (0, 2, 4)

    def half(i, h):
        n = (q_cols // 2, hd, q_cols // 4)[i]
        return pl.ds(pl.multiple_of(h * n + (q_cols if i == KV else 0), n), n)

    def win(i, h):
        return (wo_in if i == O else wt_in).at[half(i, h)]

    def wref(i, h, r):
        return (wo_all if i == O else wt_all).at[r, half(i, h)]

    def w_send_own(p, which, target):
        i, h = p
        return rcopy(win(i, h), wref(i, h, me), w_own.at[which, base[i] + h], w_recv.at[me, base[i] + h],
                     target)

    def w_wait(p, r):
        i, h = p
        ref = wref(i, h, r)
        rcopy(ref, ref, w_own.at[0, 0], w_recv.at[r, base[i] + h], sib).wait_recv()

    def w_to_sib(p, r, slot):
        i, h = p
        return rcopy(wref(i, h, r), wref(i, h, r), w_sib.at[slot, base[i] + h], w_recv.at[r, base[i] + h], sib)

    def w_onward(p, r, target):
        i, h = p
        return rcopy(wref(i, h, r), wref(i, h, r), w_fwd.at[base[i] + h], w_recv.at[r, base[i] + h], target)

    def w_to_mate(p, r, slot):
        i, h = p
        return pltpu.make_async_remote_copy(
            src_ref=wref(i, h, r), dst_ref=wref(i, h, r), send_sem=w_pair.at[slot, base[i] + h],
            recv_sem=w_recv.at[r, base[i] + h], device_id=(mate, me), device_id_type=MESH)

    left, right, far = dev(-1, 0), dev(1, 0), dev(2, 0)
    L, R, F = (left, 0), (right, 1), (far, 2)
    every = [(i, h) for i in range(3) for h in range(n_cut[i])]
    if share:
        first, from_mate = [(Q, par), (KV, par)], [(Q, 1 - par), (KV, 1 - par)]
        later, o_mate = [(O, par), (O, 2), (O, 3)], (O, 1 - par)
    else:
        first, from_mate = [(Q, 0), (KV, 0), (Q, 1), (KV, 1)], []
        later, o_mate = [(O, 0), (O, 1), (O, 2), (O, 3)], None
    shared = first + later[:1]

    def got(p, src, onward=None):
        r, slot = src
        w_wait(p, r)
        if onward is not None:
            w_onward(p, r, onward).start()
        if share and any(p is q for q in shared):
            w_to_mate(p, r, slot).start()
        w_to_sib(p, r, slot).start()

    def got_mate(p, src):
        r, slot = src
        w_wait(p, r)
        w_to_sib(p, r, slot).start()

    a2a_start(0, pos_src, pos_dst)
    for p in first:
        w_send_own(p, 1, right).start()
        w_send_own(p, 2, left).start()
    for p in every:
        w_send_own(p, 0, sib).start()
    a2a_start(set_x(0), *x_fns(0))
    for p in later:
        w_send_own(p, 2, left).start()
    nt_cols = wobuf.shape[3]
    n_nt = d_model // nt_cols
    wo_cols = [slice(n * nt_cols, (n + 1) * nt_cols) for n in range(n_nt)]
    wo_stage = [pltpu.make_async_copy(wo_in.at[:, c], wobuf.at[0, n], w_loc.at[n]) for n, c in enumerate(wo_cols)]
    wo_place = [pltpu.make_async_copy(wobuf.at[0, n], wo_all.at[me, :, c], w_loc.at[n]) for n, c in enumerate(wo_cols)]
    for c in wo_stage:
        c.start()
    a2a_wait(0, pos_src, pos_dst)

    blk = 128
    lane = lax.broadcasted_iota(jnp.int32, (blk, hd), 1)

    def table_step(b, _):
        rs = pl.ds(pl.multiple_of(b * blk, blk), blk)
        for j in range(n_seq):
            ang = posbuf[rs, j:j + 1] * invf[...]
            cs = jnp.cos(ang)
            sn = jnp.sin(ang)
            sn = jnp.where(lane < hd // 2, -sn, sn)
            qcos[j, :, rs] = (cs * qgain[0:1, :]).T
            qsin[j, :, rs] = (sn * qgain[1:2, :]).T
            kcos[j, :, rs] = (cs * kgain[0:1, :]).T
            ksin[j, :, rs] = (sn * kgain[1:2, :]).T
        return 0

    lax.fori_loop(0, seq // blk, table_step, 0)

    for p in first:
        got(p, L, right)
        got(p, R)
    a2a_start(set_x(1), *x_fns(1))
    for p in later:
        w_send_own(p, 1, right).start()

    def wait_all(arrays, r):
        for i in arrays:
            for h in range(n_cut[i]):
                w_wait((i, h), r)

    def stage(s):
        @pl.when(s == 2)
        def _():
            for p in from_mate[:1]:
                got_mate(p, L)
                got_mate(p, R)
            for p in from_mate[1:]:
                got_mate(p, L)

        @pl.when(s == 3)
        def _():
            wait_all((Q, KV), dev(-1, 1))
            got(first[0], F)

        @pl.when(s == 4)
        def _():
            for p in from_mate[1:]:
                got_mate(p, R)
            for p in first[1:]:
                got(p, F)

        @pl.when(s == 5)
        def _():
            wait_all((Q, KV), dev(1, 1))

        @pl.when(s == 6)
        def _():
            for p in later:
                got(p, R, left)
            a2a_start(set_x(2), *x_fns(2))
            a2a_start(set_x(3), *x_fns(3))
            for p in from_mate:
                got_mate(p, F)

        @pl.when(s == 7)
        def _():
            wait_all((Q, KV), dev(2, 1))

    def gid(s):
        m = s // 2
        return ((chip + 3 * m * (m + 1) // 2) % chips) * 2 + (core + s) % 2

    def load_w(g, slot):
        return [pltpu.make_async_copy(wt_all.at[g], wtb.at[slot], ld_sem.at[slot])]

    def load_wo(nt, slot):
        return pltpu.make_async_copy(wo_all.at[:, :, pl.ds(pl.multiple_of(nt * nt_cols, nt_cols), nt_cols)],
                                     wobuf.at[slot], wo_sem.at[slot])

    scale2 = (hd ** -0.5) * LOG2E
    n_blk = seq // blk
    key_i = lax.broadcasted_iota(jnp.int32, (blk, 2 * blk), 0)
    qry_i = lax.broadcasted_iota(jnp.int32, (blk, 2 * blk), 1) % blk
    tri = key_i <= qry_i

    def norm_rope(row, ls, cos, sin):
        mid = hd // 2
        u1 = qkvt[row:row + mid, ls].astype(jnp.float32)
        u2 = qkvt[row + mid:row + hd, ls].astype(jnp.float32)
        r = lax.rsqrt(jnp.sum(u1 * u1 + u2 * u2, axis=0, keepdims=True) * (1.0 / hd) + EPS)
        return ((u1 * cos[:mid] + u2 * sin[:mid]) * r, (u2 * cos[mid:] + u1 * sin[mid:]) * r)

    def project(slot):
        qkvt[...] = lax.dot_general(wtb[slot], nbuf[...], (((1,), (1,)), ((), ())),
                                    preferred_element_type=jnp.float32).astype(jnp.bfloat16)

    def rope(j):
        mid = hd // 2
        for b in range(n_blk):
            ls = slice(b * blk, (b + 1) * blk)
            o1, o2 = norm_rope(q_cols, ls, kcos[j, :, ls], ksin[j, :, ls])
            ks[ls, :] = jnp.concatenate([o1, o2], axis=0).T.astype(jnp.bfloat16)
            cos, sin = qcos[j, :, ls], qsin[j, :, ls]
            for h in range(n_heads):
                o1, o2 = norm_rope(h * hd, ls, cos, sin)
                qt[h * hd:h * hd + mid, ls] = o1.astype(jnp.bfloat16)
                qt[h * hd + mid:(h + 1) * hd, ls] = o2.astype(jnp.bfloat16)
        vt[...] = qkvt[q_cols + hd:, :]

    def attend_chunk(j, g, i, h):
        kl = (i + 1) * blk
        q2 = jnp.concatenate([qt[(h + k) * hd:(h + k + 1) * hd, i * blk:kl] for k in range(2)], axis=1)
        s = jnp.dot(ks[:kl, :], q2, preferred_element_type=jnp.float32)
        diag = jnp.where(tri, s[i * blk:, :], -jnp.inf)
        s = diag if i == 0 else jnp.concatenate([s[:i * blk, :], diag], axis=0)
        peak = jnp.max(s, axis=0, keepdims=True)
        e = jnp.exp2((s - peak) * scale2)
        inv = 1.0 / jnp.sum(e, axis=0, keepdims=True)
        p = (e * inv).astype(jnp.bfloat16)
        o = jnp.dot(vt[:, :kl], p, preferred_element_type=jnp.float32)
        for k in range(2):
            obuf[j % 2, i * blk:kl, pl.ds(pl.multiple_of(g * q_cols + (h + k) * hd, hd), hd)] = (
                o[:, k * blk:(k + 1) * blk].T.astype(jnp.bfloat16))

    def project_pieces(slot):
        m_cut, k_cut = qkvt.shape[0] // 2, d_model // 10
        for m in range(2):
            ms = slice(m * m_cut, (m + 1) * m_cut)
            acc = None
            for k in range(10):
                kc = slice(k * k_cut, (k + 1) * k_cut)
                part = lax.dot_general(wtb[slot, ms, kc], nbuf[:, kc], (((1,), (1,)), ((), ())),
                                       preferred_element_type=jnp.float32)
                acc = part if acc is None else acc + part
                if k + 1 == 10:
                    qkvt[ms, :] = acc.astype(jnp.bfloat16)
                yield

    def attend_and_project(j, g, slot):
        todo = [(i, h) for i in (0, 1, 2, 3) for h in range(0, n_heads, 2)]
        pieces = 2 * 10
        done = 0
        steps = project_pieces(slot)
        for n, (i, h) in enumerate(todo):
            want = min(pieces, -(-pieces * (n + 1 + 0) // len(todo)))
            while done < want:
                next(steps)
                done += 1
            attend_chunk(j, g, i, h)
        for _ in steps:
            pass

    n_grp = n_tp
    n_units = n_seq * n_grp

    def normalise(j):
        a2a_wait(set_x(j), *x_fns(j))

        def n_step(r, _):
            rs = rows(r)
            xv = xbuf[j, rs, :].astype(jnp.float32)
            ms = jnp.mean(xv * xv, axis=-1, keepdims=True)
            nbuf[rs, :] = (xv * lax.rsqrt(ms + EPS) * ngain[...]).astype(jnp.bfloat16)
            return 0

        lax.fori_loop(0, n_tp, n_step, 0)

    def out_proj(j):
        def out_step(nt, _):
            ws = nt % 2
            load_wo(nt, ws).wait()

            @pl.when(nt + 1 < n_nt)
            def _():
                load_wo(nt + 1, 1 - ws).start()

            cs = pl.ds(pl.multiple_of(nt * nt_cols, nt_cols), nt_cols)
            acc = jnp.dot(obuf[j % 2], wobuf[ws].reshape(n_tp * q_cols, nt_cols), preferred_element_type=jnp.float32)
            xbuf[j, :, cs] = (xbuf[j, :, cs].astype(jnp.float32) + acc).astype(jnp.bfloat16)
            return 0

        load_wo(0, 0).start()
        lax.fori_loop(0, n_nt, out_step, 0)
        a2a_start(set_y(j), *y_fns(j))

    own_load = pltpu.make_async_copy(wt_in, wtb.at[0], ld_sem.at[0])
    own_load.start()
    wait_all((Q, KV), sib)
    for c in load_w(gid(1), 1):
        c.start()
    normalise(0)
    own_load.wait()
    own_place = pltpu.make_async_copy(wtb.at[0], wt_all.at[me], ld_sem.at[0])
    own_place.start()
    for c in wo_stage:
        c.wait()
    for c in wo_place:
        c.start()
    project(0)
    own_place.wait()
    for c in wo_place:
        c.wait()

    def step(t, _):
        j, s = t // n_grp, t % n_grp
        u = t + 1

        @pl.when(j == 0)
        def _():
            stage(s + 2)

        @pl.when(jnp.logical_and(j == 1, s == 0))
        def _():
            got(later[0], L)
            got(later[0], F)

        @pl.when(jnp.logical_and(j == 1, s == 3))
        def _():
            for p in later[1:]:
                got(p, L)
                got(p, F)
            if share:
                for src in (R, L, F):
                    got_mate(o_mate, src)

        @pl.when(u + 1 < n_units)
        def _():
            for c in load_w(gid((u + 1) % n_grp), (u + 1) % 2):
                c.start()

        @pl.when(u < n_units)
        def _():
            for c in load_w(gid(u % n_grp), u % 2):
                c.wait()

        @pl.when(s == n_grp - 1)
        def _():
            @pl.when(u < n_units)
            def _():
                normalise(j + 1)

        rope(j)
        attend_and_project(j, gid(s), u % 2)

        @pl.when(jnp.logical_and(j == 1, s == n_grp - 1))
        def _():
            wait_all((O,), sib)
            for dc in (-1, 1, 2):
                wait_all((O,), dev(dc, 1))

        @pl.when(jnp.logical_and(j > 0, s == n_grp - 1))
        def _():
            def turn(jj, _):
                out_proj(jj)
                return 0

            lax.fori_loop(j * ((j + 2) // 4), j + 1, turn, 0)

        return 0

    lax.fori_loop(0, n_units, step, 0)

    for p in every:
        w_send_own(p, 0, sib).wait_send()
        for slot, r in enumerate((left, right, far)):
            w_to_sib(p, r, slot).wait_send()
    for p in first + later:
        w_send_own(p, 1, right).wait_send()
        w_send_own(p, 2, left).wait_send()
    for p in first:
        w_onward(p, left, right).wait_send()
    for p in later:
        w_onward(p, right, left).wait_send()
    if share:
        for p in shared:
            for slot, r in enumerate((left, right, far)):
                w_to_mate(p, r, slot).wait_send()
    a2a_wait_sends(0, pos_src, pos_dst)

    def end_step(j, _):
        a2a_wait_sends(set_x(j), *x_fns(j))
        a2a_wait(set_y(j), *y_fns(j))
        a2a_wait_sends(set_y(j), *y_fns(j))
        return 0

    lax.fori_loop(0, n_seq, end_step, 0)


def gain_rows(gain):
    g = gain.astype(jnp.float32)
    return jnp.stack([g, jnp.roll(g, g.shape[0] // 2)])


def solution(mesh):
    n_tp = mesh.shape['tp']

    def local_block(x_loc, pos_loc, norm_gain, w_q, w_k, w_v, q_gain, k_gain, w_o):
        batch, piece, d_model = x_loc.shape
        hd = q_gain.shape[0]
        q_cols = w_q.shape[1]
        n_seq = batch // n_tp
        seq = piece * n_tp
        f32, bf16 = jnp.float32, jnp.bfloat16
        pos = pos_loc.astype(f32).reshape(n_tp, n_seq, piece).transpose(0, 2, 1)
        pos = jnp.pad(pos, ((0, 0), (0, 0), (0, hd - n_seq)))
        inv_freq = THETA ** (-(jnp.arange(hd // 2, dtype=f32) * (2.0 / hd)))
        invf = jnp.concatenate([inv_freq, inv_freq])[None, :]
        any_spec = pl.BlockSpec(memory_space=pl.ANY)
        vmem = pl.BlockSpec(memory_space=pltpu.VMEM)
        nt_cols = 512
        dma = pltpu.SemaphoreType.DMA
        n_sets = 1 + 2 * n_seq
        w_t = jnp.concatenate([w_q, w_k, w_v], axis=1).T
        res = pl.pallas_call(
            body,
            name='attn_block',
            out_shape=[
                jax.ShapeDtypeStruct((batch, piece, d_model), bf16),
                jax.ShapeDtypeStruct((n_tp,) + w_t.shape, bf16),
                jax.ShapeDtypeStruct((n_tp,) + w_o.shape, bf16),
            ],
            in_specs=[any_spec, any_spec, vmem, vmem, vmem, vmem, any_spec, any_spec],
            out_specs=[any_spec] * 3,
            scratch_shapes=[
                pltpu.VMEM((n_seq, seq, d_model), bf16),
                pltpu.VMEM((seq, d_model), bf16),
                pltpu.VMEM((2, seq, n_tp * q_cols), bf16),
                pltpu.VMEM((2,) + w_t.shape, bf16),
                pltpu.VMEM((2, n_tp, q_cols, nt_cols), bf16),
                pltpu.VMEM((q_cols + 2 * hd, seq), bf16),
                pltpu.VMEM((q_cols, seq), bf16),
                pltpu.VMEM((seq, hd), bf16),
                pltpu.VMEM((hd, seq), bf16),
                pltpu.VMEM((n_seq, hd, seq), f32),
                pltpu.VMEM((n_seq, hd, seq), f32),
                pltpu.VMEM((n_seq, hd, seq), f32),
                pltpu.VMEM((n_seq, hd, seq), f32),
                pltpu.VMEM((seq, hd), f32),
                dma((n_sets, n_tp - 1)),
                dma((n_sets, n_tp)),
                dma((3, 8)),
                dma((8,)),
                dma((3, 8)),
                dma((3, 8)),
                dma((n_tp, 8)),
                dma((8,)),
                dma((2,)),
                dma((2,)),
            ],
            compiler_params=pltpu.CompilerParams(
                collective_id=0, has_side_effects=True, vmem_limit_bytes=62 * 1024 * 1024),
        )(x_loc, pos, invf, norm_gain.astype(f32)[None, :], gain_rows(q_gain), gain_rows(k_gain), w_t, w_o)
        return res[0]

    return jax.shard_map(
        local_block, mesh=mesh,
        in_specs=(P('dp', 'tp', None), P('dp', 'tp'), P(None), P(None, 'tp'), P(None, 'tp'), P(None, 'tp'),
                  P(None), P(None), P('tp', None)),
        out_specs=P('dp', 'tp', None), check_vma=False)
```

```python
import jax
import jax.numpy as jnp
from jax import lax
from jax.experimental import pallas as pl
from jax.experimental.pallas import tpu as pltpu
from jax.sharding import PartitionSpec as P

EPS = 1e-6
THETA = 1000000.0
MESH = pl.DeviceIdType.MESH
LOG2E = 1.4426950408889634


SHARE = True


def body(x_in, pos_in, invf, ngain, qgain, kgain, wt_in, wo_in,
         out, wt_all, wo_all,
         xbuf, nbuf, obuf, wtb, wobuf, qkvt, qt, ks, vt, qcos, qsin, kcos, ksin, posbuf,
         a_send, a_recv, w_own, w_fwd, w_sib, w_pair, w_recv, w_loc, ld_sem, wo_sem):
    d_model = nbuf.shape[1]
    seq = nbuf.shape[0]
    n_seq = xbuf.shape[0]
    hd = ks.shape[1]
    q_cols = qt.shape[0]
    n_heads = q_cols // hd
    n_tp = wt_all.shape[0]
    n_dp = lax.axis_size('dp')
    share = SHARE and n_dp % 2 == 0
    chips = n_tp // 2
    piece = seq // n_tp
    dp_i = lax.axis_index('dp')
    me = lax.axis_index('tp')
    chip = me // 2
    core = me % 2

    def dev(dc, dk):
        return ((chip + dc + chips) % chips) * 2 + (core + dk) % 2

    sib = dev(0, 1)

    def rcopy(src, dst, ssem, rsem, target):
        return pltpu.make_async_remote_copy(src_ref=src, dst_ref=dst, send_sem=ssem, recv_sem=rsem,
                                            device_id=(dp_i, target), device_id_type=MESH)

    bar = pltpu.get_barrier_semaphore()
    near = [dev(dc, dk) for dc in (-1, 1, 2) for dk in (0, 1)] + [sib]
    for t in near:
        pl.semaphore_signal(bar, inc=1, device_id=(dp_i, t), device_id_type=MESH)
    par = dp_i % 2
    mate = dp_i + 1 - 2 * par
    if share:
        pl.semaphore_signal(bar, inc=1, device_id=(mate, me), device_id_type=MESH)
    pl.semaphore_wait(bar, len(near) + (1 if share else 0))

    def rows(r):
        return pl.ds(pl.multiple_of(r * piece, piece), piece)

    others = ((2, 0), (2, 1), (1, 0), (1, 1), (-1, 0), (-1, 1), (0, 1))

    def a2a_direct(a, src, dst):
        return [rcopy(src(dev(*o)), dst(me, dev(*o)), a_send.at[a, n], a_recv.at[a, me], dev(*o))
                for n, o in enumerate(others)]

    def a2a_local(a, src, dst):
        return pltpu.make_async_copy(src(me), dst(me, me), a_recv.at[a, me])

    def a2a_start(a, src, dst):
        for c in a2a_direct(a, src, dst):
            c.start()
        a2a_local(a, src, dst).start()

    def a2a_wait(a, src, dst):
        a2a_local(a, src, dst).wait()
        for o in others:
            r = dev(*o)
            ref = dst(r, me)
            rcopy(ref, ref, a_send.at[a, 0], a_recv.at[a, r], sib).wait_recv()

    def a2a_wait_sends(a, src, dst):
        for c in a2a_direct(a, src, dst):
            c.wait_send()

    def pos_src(r):
        return pos_in.at[r]

    def pos_dst(r, to):
        return posbuf.at[rows(r)]

    def x_fns(j):
        return (lambda r: x_in.at[r * n_seq + j],
                lambda r, to: xbuf.at[j, rows(r)])

    def y_fns(j, nt):
        cs = pl.ds(pl.multiple_of(nt * nt_cols, nt_cols), nt_cols)
        return (lambda r: xbuf.at[j, rows(r), cs],
                lambda r, to: out.at[r * n_seq + j, :, cs])

    def set_x(j):
        return 1 + j

    def set_y(j, nt):
        return 1 + n_seq + j * n_nt + nt

    Q, KV, O = range(3)

    n_cut = (2, 2, 4)
    base = (0, 2, 4)

    def half(i, h):
        n = (q_cols // 2, hd, q_cols // 4)[i]
        return pl.ds(pl.multiple_of(h * n + (q_cols if i == KV else 0), n), n)

    def win(i, h):
        return (wo_in if i == O else wt_in).at[half(i, h)]

    def wref(i, h, r):
        return (wo_all if i == O else wt_all).at[r, half(i, h)]

    def w_send_own(p, which, target):
        i, h = p
        return rcopy(win(i, h), wref(i, h, me), w_own.at[which, base[i] + h], w_recv.at[me, base[i] + h],
                     target)

    def w_wait(p, r):
        i, h = p
        ref = wref(i, h, r)
        rcopy(ref, ref, w_own.at[0, 0], w_recv.at[r, base[i] + h], sib).wait_recv()

    def w_to_sib(p, r, slot):
        i, h = p
        return rcopy(wref(i, h, r), wref(i, h, r), w_sib.at[slot, base[i] + h], w_recv.at[r, base[i] + h], sib)

    def w_onward(p, r, target):
        i, h = p
        return rcopy(wref(i, h, r), wref(i, h, r), w_fwd.at[base[i] + h], w_recv.at[r, base[i] + h], target)

    def w_to_mate(p, r, slot):
        i, h = p
        return pltpu.make_async_remote_copy(
            src_ref=wref(i, h, r), dst_ref=wref(i, h, r), send_sem=w_pair.at[slot, base[i] + h],
            recv_sem=w_recv.at[r, base[i] + h], device_id=(mate, me), device_id_type=MESH)

    left, right, far = dev(-1, 0), dev(1, 0), dev(2, 0)
    L, R, F = (left, 0), (right, 1), (far, 2)
    every = [(i, h) for i in range(3) for h in range(n_cut[i])]
    if share:
        first, from_mate = [(Q, par), (KV, par)], [(Q, 1 - par), (KV, 1 - par)]
        later, o_mate = [(O, par), (O, 2), (O, 3)], (O, 1 - par)
    else:
        first, from_mate = [(Q, 0), (KV, 0), (Q, 1), (KV, 1)], []
        later, o_mate = [(O, 0), (O, 1), (O, 2), (O, 3)], None
    shared = first + later[:1]

    def got(p, src, onward=None):
        r, slot = src
        w_wait(p, r)
        if onward is not None:
            w_onward(p, r, onward).start()
        if share and any(p is q for q in shared):
            w_to_mate(p, r, slot).start()
        w_to_sib(p, r, slot).start()

    def got_mate(p, src):
        r, slot = src
        w_wait(p, r)
        w_to_sib(p, r, slot).start()

    a2a_start(0, pos_src, pos_dst)
    for p in first:
        w_send_own(p, 1, right).start()
        w_send_own(p, 2, left).start()
    for p in every:
        w_send_own(p, 0, sib).start()
    a2a_start(set_x(0), *x_fns(0))
    for p in later:
        w_send_own(p, 2, left).start()
    nt_cols = wobuf.shape[3]
    n_nt = d_model // nt_cols
    wo_cols = [slice(n * nt_cols, (n + 1) * nt_cols) for n in range(n_nt)]
    wo_stage = [pltpu.make_async_copy(wo_in.at[:, c], wobuf.at[0, n], w_loc.at[n]) for n, c in enumerate(wo_cols)]
    wo_place = [pltpu.make_async_copy(wobuf.at[0, n], wo_all.at[me, :, c], w_loc.at[n]) for n, c in enumerate(wo_cols)]
    for c in wo_stage:
        c.start()
    a2a_wait(0, pos_src, pos_dst)

    blk = 128
    lane = lax.broadcasted_iota(jnp.int32, (blk, hd), 1)

    def turned(gain):
        return pltpu.roll(jnp.broadcast_to(gain[...], (8, hd)), hd // 2, 1)[0:1]

    q_gain2, k_gain2 = turned(qgain), turned(kgain)

    def table_step(b, _):
        rs = pl.ds(pl.multiple_of(b * blk, blk), blk)
        for j in range(n_seq):
            ang = posbuf[rs, j:j + 1] * invf[...]
            cs = jnp.cos(ang)
            sn = jnp.sin(ang)
            sn = jnp.where(lane < hd // 2, -sn, sn)
            qcos[j, :, rs] = (cs * qgain[...]).T
            qsin[j, :, rs] = (sn * q_gain2).T
            kcos[j, :, rs] = (cs * kgain[...]).T
            ksin[j, :, rs] = (sn * k_gain2).T
        return 0

    lax.fori_loop(0, seq // blk, table_step, 0)

    for p in first:
        got(p, L, right)
        got(p, R)
    a2a_start(set_x(1), *x_fns(1))
    for p in later:
        w_send_own(p, 1, right).start()

    def wait_all(arrays, r):
        for i in arrays:
            for h in range(n_cut[i]):
                w_wait((i, h), r)

    def stage(s):
        @pl.when(s == 2)
        def _():
            for p in from_mate[:1]:
                got_mate(p, L)
                got_mate(p, R)
            for p in from_mate[1:]:
                got_mate(p, L)

        @pl.when(s == 3)
        def _():
            wait_all((Q, KV), dev(-1, 1))
            got(first[0], F)

        @pl.when(s == 4)
        def _():
            for p in from_mate[1:]:
                got_mate(p, R)
            for p in first[1:]:
                got(p, F)

        @pl.when(s == 5)
        def _():
            wait_all((Q, KV), dev(1, 1))

        @pl.when(s == 6)
        def _():
            for p in later:
                got(p, R, left)
            a2a_start(set_x(2), *x_fns(2))
            a2a_start(set_x(3), *x_fns(3))
            for p in from_mate:
                got_mate(p, F)

        @pl.when(s == 7)
        def _():
            wait_all((Q, KV), dev(2, 1))

    def gid(s):
        m = s // 2
        return ((chip + 3 * m * (m + 1) // 2) % chips) * 2 + (core + s) % 2

    def load_w(g, slot):
        return [pltpu.make_async_copy(wt_all.at[g], wtb.at[slot], ld_sem.at[slot])]

    def load_wo(nt, slot):
        return pltpu.make_async_copy(wo_all.at[:, :, pl.ds(pl.multiple_of(nt * nt_cols, nt_cols), nt_cols)],
                                     wobuf.at[slot], wo_sem.at[slot])

    scale2 = (hd ** -0.5) * LOG2E
    n_blk = seq // blk
    key_i = lax.broadcasted_iota(jnp.int32, (blk, 2 * blk), 0)
    qry_i = lax.broadcasted_iota(jnp.int32, (blk, 2 * blk), 1) % blk
    tri = key_i <= qry_i

    def norm_rope(row, ls, cos, sin):
        mid = hd // 2
        u1 = qkvt[row:row + mid, ls].astype(jnp.float32)
        u2 = qkvt[row + mid:row + hd, ls].astype(jnp.float32)
        r = lax.rsqrt(jnp.sum(u1 * u1 + u2 * u2, axis=0, keepdims=True) * (1.0 / hd) + EPS)
        return ((u1 * cos[:mid] + u2 * sin[:mid]) * r, (u2 * cos[mid:] + u1 * sin[mid:]) * r)

    def project(slot):
        qkvt[...] = lax.dot_general(wtb[slot], nbuf[...], (((1,), (1,)), ((), ())),
                                    preferred_element_type=jnp.float32).astype(jnp.bfloat16)

    def rope(j):
        mid = hd // 2
        for b in range(n_blk):
            ls = slice(b * blk, (b + 1) * blk)
            o1, o2 = norm_rope(q_cols, ls, kcos[j, :, ls], ksin[j, :, ls])
            ks[ls, :] = jnp.concatenate([o1, o2], axis=0).T.astype(jnp.bfloat16)
            cos, sin = qcos[j, :, ls], qsin[j, :, ls]
            for h in range(n_heads):
                o1, o2 = norm_rope(h * hd, ls, cos, sin)
                qt[h * hd:h * hd + mid, ls] = o1.astype(jnp.bfloat16)
                qt[h * hd + mid:(h + 1) * hd, ls] = o2.astype(jnp.bfloat16)
        vt[...] = qkvt[q_cols + hd:, :]

    def attend_chunk(j, g, i, h):
        kl = (i + 1) * blk
        q2 = jnp.concatenate([qt[(h + k) * hd:(h + k + 1) * hd, i * blk:kl] for k in range(2)], axis=1)
        s = jnp.dot(ks[:kl, :], q2, preferred_element_type=jnp.float32)
        diag = jnp.where(tri, s[i * blk:, :], -jnp.inf)
        s = diag if i == 0 else jnp.concatenate([s[:i * blk, :], diag], axis=0)
        peak = jnp.max(s, axis=0, keepdims=True)
        e = jnp.exp2((s - peak) * scale2)
        inv = 1.0 / jnp.sum(e, axis=0, keepdims=True)
        p = (e * inv).astype(jnp.bfloat16)
        o = jnp.dot(vt[:, :kl], p, preferred_element_type=jnp.float32)
        for k in range(2):
            obuf[j % 2, i * blk:kl, pl.ds(pl.multiple_of(g * q_cols + (h + k) * hd, hd), hd)] = (
                o[:, k * blk:(k + 1) * blk].T.astype(jnp.bfloat16))

    def project_pieces(slot):
        m_cut, k_cut = qkvt.shape[0] // 2, d_model // 10
        for m in range(2):
            ms = slice(m * m_cut, (m + 1) * m_cut)
            acc = None
            for k in range(10):
                kc = slice(k * k_cut, (k + 1) * k_cut)
                part = lax.dot_general(wtb[slot, ms, kc], nbuf[:, kc], (((1,), (1,)), ((), ())),
                                       preferred_element_type=jnp.float32)
                acc = part if acc is None else acc + part
                if k + 1 == 10:
                    qkvt[ms, :] = acc.astype(jnp.bfloat16)
                yield

    def attend_and_project(j, g, slot):
        todo = [(i, h) for i in (0, 1, 2, 3) for h in range(0, n_heads, 2)]
        pieces = 2 * 10
        done = 0
        steps = project_pieces(slot)
        for n, (i, h) in enumerate(todo):
            want = min(pieces, -(-pieces * (n + 1 + 0) // len(todo)))
            while done < want:
                next(steps)
                done += 1
            attend_chunk(j, g, i, h)
        for _ in steps:
            pass

    n_grp = n_tp
    n_units = n_seq * n_grp

    def normalise(j):
        a2a_wait(set_x(j), *x_fns(j))

        def n_step(r, _):
            rs = rows(r)
            xv = xbuf[j, rs, :].astype(jnp.float32)
            ms = jnp.mean(xv * xv, axis=-1, keepdims=True)
            nbuf[rs, :] = (xv * lax.rsqrt(ms + EPS) * ngain[...]).astype(jnp.bfloat16)
            return 0

        lax.fori_loop(0, n_tp, n_step, 0)

    def out_proj(j):
        def out_step(nt, _):
            ws = nt % 2
            load_wo(nt, ws).wait()

            @pl.when(nt + 1 < n_nt)
            def _():
                load_wo(nt + 1, 1 - ws).start()

            cs = pl.ds(pl.multiple_of(nt * nt_cols, nt_cols), nt_cols)
            acc = jnp.dot(obuf[j % 2], wobuf[ws].reshape(n_tp * q_cols, nt_cols), preferred_element_type=jnp.float32)
            xbuf[j, :, cs] = (xbuf[j, :, cs].astype(jnp.float32) + acc).astype(jnp.bfloat16)
            a2a_start(set_y(j, nt), *y_fns(j, nt))
            return 0

        load_wo(0, 0).start()
        lax.fori_loop(0, n_nt, out_step, 0)

    own_load = pltpu.make_async_copy(wt_in, wtb.at[0], ld_sem.at[0])
    own_load.start()
    wait_all((Q, KV), sib)
    for c in load_w(gid(1), 1):
        c.start()
    normalise(0)
    own_load.wait()
    own_place = pltpu.make_async_copy(wtb.at[0], wt_all.at[me], ld_sem.at[0])
    own_place.start()
    for c in wo_stage:
        c.wait()
    for c in wo_place:
        c.start()
    project(0)
    own_place.wait()
    for c in wo_place:
        c.wait()

    def step(t, _):
        j, s = t // n_grp, t % n_grp
        u = t + 1

        @pl.when(j == 0)
        def _():
            stage(s + 2)

        @pl.when(jnp.logical_and(j == 1, s == 0))
        def _():
            got(later[0], L)
            got(later[0], F)

        @pl.when(jnp.logical_and(j == 1, s == 3))
        def _():
            for p in later[1:]:
                got(p, L)
                got(p, F)
            if share:
                for src in (R, L, F):
                    got_mate(o_mate, src)

        @pl.when(u + 1 < n_units)
        def _():
            for c in load_w(gid((u + 1) % n_grp), (u + 1) % 2):
                c.start()

        @pl.when(u < n_units)
        def _():
            for c in load_w(gid(u % n_grp), u % 2):
                c.wait()

        @pl.when(s == n_grp - 1)
        def _():
            @pl.when(u < n_units)
            def _():
                normalise(j + 1)

        rope(j)
        attend_and_project(j, gid(s), u % 2)

        @pl.when(jnp.logical_and(j == 1, s == n_grp - 1))
        def _():
            wait_all((O,), sib)
            for dc in (-1, 1, 2):
                wait_all((O,), dev(dc, 1))

        @pl.when(jnp.logical_and(j > 0, s == n_grp - 1))
        def _():
            def turn(jj, _):
                out_proj(jj)
                return 0

            lax.fori_loop(j * ((j + 2) // 4), j + 1, turn, 0)

        return 0

    lax.fori_loop(0, n_units, step, 0)

    for p in every:
        w_send_own(p, 0, sib).wait_send()
        for slot, r in enumerate((left, right, far)):
            w_to_sib(p, r, slot).wait_send()
    for p in first + later:
        w_send_own(p, 1, right).wait_send()
        w_send_own(p, 2, left).wait_send()
    for p in first:
        w_onward(p, left, right).wait_send()
    for p in later:
        w_onward(p, right, left).wait_send()
    if share:
        for p in shared:
            for slot, r in enumerate((left, right, far)):
                w_to_mate(p, r, slot).wait_send()
    a2a_wait_sends(0, pos_src, pos_dst)

    def end_step(j, _):
        a2a_wait_sends(set_x(j), *x_fns(j))

        def end_cols(nt, _):
            a2a_wait(set_y(j, nt), *y_fns(j, nt))
            a2a_wait_sends(set_y(j, nt), *y_fns(j, nt))
            return 0

        lax.fori_loop(0, n_nt, end_cols, 0)
        return 0

    lax.fori_loop(0, n_seq, end_step, 0)


def solution(mesh):
    n_tp = mesh.shape['tp']

    def local_block(x_loc, pos_loc, norm_gain, w_q, w_k, w_v, q_gain, k_gain, w_o):
        batch, piece, d_model = x_loc.shape
        hd = q_gain.shape[0]
        q_cols = w_q.shape[1]
        n_seq = batch // n_tp
        seq = piece * n_tp
        f32, bf16 = jnp.float32, jnp.bfloat16
        pos = pos_loc.astype(f32).reshape(n_tp, n_seq, piece).transpose(0, 2, 1)
        pos = jnp.pad(pos, ((0, 0), (0, 0), (0, hd - n_seq)))
        inv_freq = THETA ** (-(jnp.arange(hd // 2, dtype=f32) * (2.0 / hd)))
        invf = jnp.concatenate([inv_freq, inv_freq])[None, :]
        any_spec = pl.BlockSpec(memory_space=pl.ANY)
        vmem = pl.BlockSpec(memory_space=pltpu.VMEM)
        nt_cols = 512
        dma = pltpu.SemaphoreType.DMA
        n_sets = 1 + n_seq + n_seq * (d_model // nt_cols)
        w_t = jnp.concatenate([w_q, w_k, w_v], axis=1).T
        res = pl.pallas_call(
            body,
            name='attn_block',
            out_shape=[
                jax.ShapeDtypeStruct((batch, piece, d_model), bf16),
                jax.ShapeDtypeStruct((n_tp,) + w_t.shape, bf16),
                jax.ShapeDtypeStruct((n_tp,) + w_o.shape, bf16),
            ],
            in_specs=[any_spec, any_spec, vmem, vmem, vmem, vmem, any_spec, any_spec],
            out_specs=[any_spec] * 3,
            scratch_shapes=[
                pltpu.VMEM((n_seq, seq, d_model), bf16),
                pltpu.VMEM((seq, d_model), bf16),
                pltpu.VMEM((2, seq, n_tp * q_cols), bf16),
                pltpu.VMEM((2,) + w_t.shape, bf16),
                pltpu.VMEM((2, n_tp, q_cols, nt_cols), bf16),
                pltpu.VMEM((q_cols + 2 * hd, seq), bf16),
                pltpu.VMEM((q_cols, seq), bf16),
                pltpu.VMEM((seq, hd), bf16),
                pltpu.VMEM((hd, seq), bf16),
                pltpu.VMEM((n_seq, hd, seq), f32),
                pltpu.VMEM((n_seq, hd, seq), f32),
                pltpu.VMEM((n_seq, hd, seq), f32),
                pltpu.VMEM((n_seq, hd, seq), f32),
                pltpu.VMEM((seq, hd), f32),
                dma((n_sets, n_tp - 1)),
                dma((n_sets, n_tp)),
                dma((3, 8)),
                dma((8,)),
                dma((3, 8)),
                dma((3, 8)),
                dma((n_tp, 8)),
                dma((8,)),
                dma((2,)),
                dma((2,)),
            ],
            compiler_params=pltpu.CompilerParams(
                collective_id=0, has_side_effects=True, vmem_limit_bytes=62 * 1024 * 1024),
        )(x_loc, pos, invf, norm_gain.astype(f32)[None, :], q_gain.astype(f32)[None, :], k_gain.astype(f32)[None, :], w_t, w_o)
        return res[0]

    return jax.shard_map(
        local_block, mesh=mesh,
        in_specs=(P('dp', 'tp', None), P('dp', 'tp'), P(None), P(None, 'tp'), P(None, 'tp'), P(None, 'tp'),
                  P(None), P(None), P('tp', None)),
        out_specs=P('dp', 'tp', None), check_vma=False)
```
